32 devices in a mesh: head: 4 (over z), ctx: 8 (over y, x, core).
Axes of the slice: x: 2, y: 2, z: 4, core: 2. Of those that a mesh axis runs over, the one named last changes fastest.
Arguments:
- queries: bfloat16 [8192, 4, 128], P('ctx', 'head'), may hold values from -120 to 120
- keys: bfloat16 [8192, 4, 128], P('ctx', 'head'), may hold values from -6 to 6
- values: bfloat16 [8192, 4, 128], P('ctx', 'head'), may hold values from -6 to 6
- house: bfloat16 [8192, 4, 128], P('ctx', 'head'), may hold values from -6 to 6
- rates: float32 [4, 8192], P('head', 'ctx'), may hold values from 0.0002 to 1.9, as said below
- out_weight: bfloat16 [512, 8192], P('head'), may hold values from -0.375 to 0.375
Outputs:
- attended: bfloat16 [8192, 4, 128], P('ctx', 'head')
- projected: bfloat16 [8192, 8192], P('ctx', 'head')
The draws below stay inside these ranges and needn't reach their ends.
Inputs may be any that keep to these rules, and one draw needn't show every extreme that they name: `rates`: strictly positive and below 2, so every transition is a contraction.
All inputs are finite; a program needn't handle non-finite values.
Results may differ from the reference program's by a relative error of at most 0.015.
Values may be sent and summed in bfloat16 or wider, within the bound.
A program may use at most 64 MiB of HBM per device.

```python
import jax
import jax.numpy as jnp
from jax import lax

DH = 128
DMODEL = 8192
BLOCK = 128
TOK_DEV = 1024
SHARD_ATTN_COUNT = 4
PROMPT_LENGTH = 8192
N_CTX = 8


def key_base(key):
    return jnp.clip(jax.random.normal(jax.random.fold_in(key, 31), (PROMPT_LENGTH, SHARD_ATTN_COUNT, DH), jnp.float32), -6.0, 6.0)


def draw_keys(key, part):
    return key_base(key).astype(jnp.bfloat16)


def draw_queries(key, part):
    drawn = jnp.clip(2.0 * jax.random.normal(jax.random.fold_in(key, 47), (PROMPT_LENGTH, SHARD_ATTN_COUNT, DH), jnp.float32), -12.0, 12.0)
    return drawn.astype(jnp.bfloat16)


def draw_rates(key, part):
    head_key = jax.random.fold_in(key, 61)
    jitter_key = jax.random.fold_in(key, 67)
    spike_draw_seed = jax.random.fold_in(key, 71)
    spot_key = jax.random.fold_in(key, 73)
    lowest, highest = (0.002, 0.6)
    head_rate = jnp.exp(jax.random.uniform(head_key, (SHARD_ATTN_COUNT, 1), jnp.float32, jnp.log(lowest), jnp.log(highest)))
    random_noise = jnp.exp(jax.random.uniform(jitter_key, (SHARD_ATTN_COUNT, PROMPT_LENGTH), jnp.float32, jnp.log(0.5), jnp.log(2.0)))
    spots = jax.random.randint(spot_key, (6,), 0, PROMPT_LENGTH)
    position = jnp.arange(PROMPT_LENGTH)
    struck = jnp.any(position[:, None] == spots[None, :], axis=1)
    steep_forgetting = jax.random.uniform(spike_draw_seed, (SHARD_ATTN_COUNT, PROMPT_LENGTH), jnp.float32, 0.8, 1.5)
    steady = jnp.clip(head_rate * random_noise, 0.0002, 1.9)
    return jnp.where(struck[None, :], steep_forgetting, steady).astype(jnp.float32)


def spiked(values, key, source, target, parts, factor):
    owner, partner = [(jnp.arange(values.shape[dim]) // (values.shape[dim] // parts)).reshape([-1 if axis == dim else 1 for axis in range(values.ndim)]) for dim in (source, target)]
    chosen = jax.random.permutation(key, parts)[partner]
    strong = (owner == chosen) | (owner == (partner + parts // 2) % parts)
    return jnp.where(strong, factor * values, values)


def block_scale(key, shape, split, least, largest):
    def one(dim, parts):
        steps = jax.random.uniform(jax.random.fold_in(jax.random.fold_in(key, 6), dim), (parts,), jnp.float32, least / len(split), largest / len(split))
        return jnp.repeat(jnp.exp(steps), shape[dim] // parts).reshape((-1,) + (1,) * (len(shape) - dim - 1))

    loudness = one(*split[0])
    for cut in split[1:]:
        loudness = loudness * one(*cut)
    return loudness


def centred(rng, shape, deviation, bound, pieces=(), kind=jnp.bfloat16):
    loudness = block_scale(rng, shape, pieces, -0.22, 0.18) if pieces else 1.0
    drawn = jax.random.normal(rng, shape, jnp.float32) * deviation * loudness
    return jnp.minimum(jnp.maximum(drawn, -bound), bound).astype(kind)


def heavy_noise(key, shape, spread, bound, shards, heavy, held_as=jnp.bfloat16):
    values = spread * jax.random.normal(key, shape, jnp.float32)
    if shards:
        values = values * block_scale(key, shape, shards, -0.22, 0.18)
    return jnp.clip(spiked(values, jax.random.fold_in(key, 3), *heavy), -bound, bound).astype(held_as)


def setup_inputs(seed: int = 0) -> dict:
    streams_of = jax.random.split(jax.random.key(seed), 7)
    return {
        "queries": draw_queries(jax.random.fold_in(streams_of[6], 71), 0),
        "keys": draw_keys(jax.random.fold_in(streams_of[6], 71), 0),
        "values": centred(streams_of[2], (PROMPT_LENGTH, SHARD_ATTN_COUNT, DH), 1.0, 6.0, ((0, 8), (1, 4))),
        "house": centred(streams_of[3], (PROMPT_LENGTH, SHARD_ATTN_COUNT, DH), 1.0, 6.0, ((0, 8), (1, 4))),
        "rates": draw_rates(jax.random.fold_in(streams_of[6], 71), 0),
        "out_weight": heavy_noise(streams_of[5], (SHARD_ATTN_COUNT * DH, DMODEL), (SHARD_ATTN_COUNT * DH) ** -0.5, 0.375, ((0, 4),), (0, 1, 4, 2.0)),
    }


EPSILON = 1e-06
NEGATIVE = -1e+30
PRECISE = lax.Precision.HIGHEST

def matmul(first_matrix, second_matrix):
    return jnp.matmul(first_matrix, second_matrix, precision=PRECISE)

def block_parts(query_rows, key_rows, house_rows, decays):
    length = query_rows.shape[0]
    features = query_rows.shape[1]
    row_index = lax.broadcasted_iota(jnp.int32, (length, length), 0)
    col_index = lax.broadcasted_iota(jnp.int32, (length, length), 1)
    gram_matrix = matmul(house_rows, house_rows.T)
    zero_block = jnp.zeros_like(gram_matrix)
    lower_part = jnp.where(row_index > col_index, gram_matrix, zero_block) + jnp.diag(1.0 / decays)
    identity = jnp.eye(length, dtype=query_rows.dtype)
    inverse = jax.scipy.linalg.solve_triangular(lower_part, identity, lower=True)
    left_part = jnp.where(row_index >= col_index, matmul(query_rows, house_rows.T), zero_block)
    right_part = matmul(inverse, jnp.where(row_index > col_index, matmul(house_rows, key_rows.T), zero_block))
    start_query = query_rows - matmul(matmul(left_part, inverse), house_rows)
    final_key = key_rows - matmul(right_part.T, house_rows)
    inside_mask = matmul(query_rows, key_rows.T) - matmul(left_part, right_part)
    inside_mask = jnp.where(row_index >= col_index, inside_mask, NEGATIVE)
    passage = jnp.eye(features, dtype=query_rows.dtype) - matmul(house_rows.T, matmul(inverse, house_rows))
    return (start_query, final_key, inside_mask, passage)

def shard_local(start_query, final_key, inside_mask, passage):
    blocks, length, features = start_query.shape
    rows_dev = blocks * length
    col_block = lax.broadcasted_iota(jnp.int32, (length, rows_dev), 1) // length
    anchor = jnp.zeros((), jnp.int32)

    def advance(running, element):
        moved_keys, prefix = running
        number, query_rows, key_rows, inside_rows, passage_rows = element
        across = matmul(query_rows, moved_keys.T)
        scores = jnp.where(col_block < number, across, NEGATIVE)
        scores = lax.dynamic_update_slice(scores, inside_rows, (anchor, number * length))
        carried_query = matmul(query_rows, prefix)
        moved_keys = matmul(moved_keys, passage_rows.T)
        moved_keys = lax.dynamic_update_slice(moved_keys, key_rows, (number * length, anchor))
        prefix = matmul(passage_rows, prefix)
        return ((moved_keys, prefix), (scores, carried_query))
    numbers = jnp.arange(blocks, dtype=jnp.int32)
    initial = (jnp.zeros((rows_dev, features), start_query.dtype), jnp.eye(features, dtype=start_query.dtype))
    (end_keys, transit), (scores, carried) = lax.scan(advance, initial, (numbers, start_query, final_key, inside_mask, passage))
    return (scores.reshape(rows_dev, rows_dev), carried.reshape(rows_dev, features), end_keys, transit)

def head_attention(query_all, key_all, value_all, house_all, decays):
    features = query_all.shape[1]
    blocks = PROMPT_LENGTH // BLOCK
    query_f = query_all.astype(jnp.float32) * features ** (-0.5)
    key_f = key_all.astype(jnp.float32)
    house_f = house_all.astype(jnp.float32)
    house_unit = house_f / jnp.sqrt(lax.optimization_barrier(jnp.sum(house_f * house_f, axis=1, keepdims=True)) + EPSILON)
    block_data = jax.vmap(block_parts)(query_f.reshape(blocks, BLOCK, features), key_f.reshape(blocks, BLOCK, features), house_unit.reshape(blocks, BLOCK, features), decays.reshape(blocks, BLOCK))
    per_shard = [array.reshape((N_CTX, TOK_DEV // BLOCK) + array.shape[1:]) for array in block_data]
    scores_local, carried, end_keys, transit = jax.vmap(shard_local)(*per_shard)
    stored_keys = end_keys.astype(jnp.bfloat16).astype(jnp.float32)
    value_blocks = value_all.astype(jnp.float32).reshape(N_CTX, TOK_DEV, features)
    anchor = jnp.zeros((), jnp.int32)

    def shard_rows(number):
        start_rows = lax.dynamic_index_in_dim(carried, number, 0, keepdims=False)
        own_scores = lax.dynamic_index_in_dim(scores_local, number, 0, keepdims=False)
        row_scores = jnp.full((TOK_DEV, PROMPT_LENGTH), NEGATIVE, query_f.dtype)
        row_scores = lax.dynamic_update_slice(row_scores, own_scores, (anchor, number * TOK_DEV))

        def visit_shard(offset, running):
            moving, table_scores = running
            source = number - 1 - offset
            block_keys = lax.dynamic_index_in_dim(stored_keys, source, 0, keepdims=False)
            table_scores = lax.dynamic_update_slice(table_scores, matmul(moving, block_keys.T), (anchor, source * TOK_DEV))
            moving = matmul(moving, lax.dynamic_index_in_dim(transit, source, 0, keepdims=False))
            return (moving, table_scores)
        _, row_scores = lax.fori_loop(anchor, number, visit_shard, (start_rows, row_scores))
        row_peak = lax.optimization_barrier(jnp.max(row_scores, axis=1, keepdims=True))
        weight_matrix = jnp.exp(row_scores - row_peak)
        totals = lax.optimization_barrier(jnp.sum(weight_matrix, axis=1))
        rounded = lax.optimization_barrier(weight_matrix.astype(jnp.bfloat16)).astype(jnp.float32)

        def gather_values(source, summed):
            weight_piece = lax.dynamic_slice_in_dim(rounded, source * TOK_DEV, TOK_DEV, 1)
            value_piece = lax.dynamic_index_in_dim(value_blocks, source, 0, keepdims=False)
            return summed + matmul(weight_piece, value_piece)
        summed = lax.fori_loop(anchor, number + 1, gather_values, jnp.zeros((TOK_DEV, features), query_f.dtype))
        return (summed / totals[:, None]).astype(jnp.bfloat16)
    outputs = lax.map(shard_rows, jnp.arange(N_CTX, dtype=jnp.int32))
    return outputs.reshape(PROMPT_LENGTH, features)

def reference(queries, keys, values, house, rates, out_weight):

    def select_head(number):
        return head_attention(lax.dynamic_index_in_dim(queries, number, 1, keepdims=False), lax.dynamic_index_in_dim(keys, number, 1, keepdims=False), lax.dynamic_index_in_dim(values, number, 1, keepdims=False), lax.dynamic_index_in_dim(house, number, 1, keepdims=False), lax.dynamic_index_in_dim(rates, number, 0, keepdims=False))
    per_head = lax.map(select_head, jnp.arange(SHARD_ATTN_COUNT, dtype=jnp.int32))
    attended = jnp.transpose(per_head, (1, 0, 2))
    flattened = attended.reshape(PROMPT_LENGTH, SHARD_ATTN_COUNT * DH)
    projected = matmul(flattened.astype(jnp.float32), out_weight.astype(jnp.float32))
    return (attended, projected.astype(jnp.bfloat16))
```

```python
import functools

import jax
import jax.numpy as jnp
from jax import lax
from jax.experimental import pallas as pl
from jax.experimental.pallas import tpu as pltpu
from jax.sharding import PartitionSpec as P

EPSILON = 1e-06
NEGATIVE = -1e30
MESH = pl.DeviceIdType.MESH
F32 = jnp.float32
BF16 = jnp.bfloat16
NT = (((1,), (1,)), ((), ()))


def mm(a, b):
    return jnp.dot(a, b, preferred_element_type=F32)


def split(x):
    high = x.astype(BF16)
    return high, (x - high.astype(F32)).astype(BF16)


def dot3(a, b):
    (ah, al), (bh, bl) = split(a), split(b)
    if a.shape[1] <= 128:
        return mm(jnp.concatenate([ah, al], 1), jnp.concatenate([bh, bh], 0)) + mm(ah, bl)
    return mm(ah, bh) + mm(al, bh) + mm(ah, bl)


def kernel(
    n_ctx, n_head, block, halves,
    q_ref, k_ref, v_ref, h_ref, rates_ref, w_ref,
    flat_ref, cols_ref,
    kall, vall, wbuf, att, nmat, inv, moved, mov, acc, peak, total,
    v_ssem, v_fsem, v_rsem, k_ssem, k_fsem, k_rsem,
    w_ssem, w_rsem, wf_ssem, wf_rsem, a_ssem, a_rsem, a_fsem, own_sem, out_sem,
):
    me = lax.axis_index("ctx")
    head = lax.axis_index("head")
    rows, feat = q_ref.shape
    blocks = rows // block
    width = wbuf.shape[1]
    half_width = width // 2
    scale = feat ** (-0.5)
    odd = lax.rem(me, 2)
    partner = me + 1 - 2 * odd
    later_pairs = (n_ctx - 1 - me) // 2
    earlier_pairs = me // 2
    span = rows // halves

    barrier = pltpu.get_barrier_semaphore()
    for step in range(1, n_ctx):
        pl.semaphore_signal(barrier, inc=1, device_id={"ctx": lax.rem(me + step, n_ctx)}, device_id_type=MESH)
    for step in range(1, n_head):
        pl.semaphore_signal(barrier, inc=1, device_id={"head": lax.rem(head + step, n_head)}, device_id_type=MESH)
    pl.semaphore_wait(barrier, n_ctx + n_head - 2)

    def slab(buf, owner, send, recv, peer):
        return pltpu.make_async_remote_copy(
            src_ref=buf.at[owner], dst_ref=buf.at[owner], send_sem=send, recv_sem=recv.at[owner],
            device_id={"ctx": peer}, device_id_type=MESH)

    def v_copy(owner, peer):
        return slab(vall, owner, v_ssem.at[peer], v_rsem, peer)

    def k_copy(owner, peer):
        return slab(kall, owner, k_ssem.at[peer], k_rsem, peer)

    def v_forward(owner):
        return slab(vall, owner, v_fsem.at[owner], v_rsem, partner)

    def k_forward(owner):
        return slab(kall, owner, k_fsem.at[owner], k_rsem, partner)

    def to_later(copy, action):
        def go(i, carry):
            action(copy(me, me + 2 * (later_pairs - i)))
            return carry
        lax.fori_loop(0, later_pairs, go, 0)

        @pl.when(odd == 0)
        def _():
            action(copy(me, me + 1))

    def half_cols(base, which):
        return pl.ds(pl.multiple_of(base + which * half_width, 128), half_width)

    def w_copy(owner, peer):
        return pltpu.make_async_remote_copy(
            src_ref=w_ref.at[:, half_cols(peer * width, odd)],
            dst_ref=wbuf.at[pl.ds(pl.multiple_of(owner * feat, 128), feat), half_cols(0, odd)],
            send_sem=w_ssem.at[peer], recv_sem=w_rsem.at[owner],
            device_id={"head": peer}, device_id_type=MESH)

    def w_swap(owner, which):
        part = wbuf.at[pl.ds(pl.multiple_of(owner * feat, 128), feat), half_cols(0, which)]
        return pltpu.make_async_remote_copy(
            src_ref=part, dst_ref=part, send_sem=wf_ssem.at[owner], recv_sem=wf_rsem.at[owner],
            device_id={"ctx": partner}, device_id_type=MESH)

    def a_rows(part):
        return pl.ds(part * span, span)

    def a_cols(owner):
        return pl.ds(pl.multiple_of(owner * feat, 128), feat)

    def a_copy(owner, peer, part):
        return pltpu.make_async_remote_copy(
            src_ref=att.at[a_rows(part), :], dst_ref=flat_ref.at[a_rows(part), a_cols(owner)],
            send_sem=a_ssem.at[part, peer], recv_sem=a_rsem.at[part, owner],
            device_id={"head": peer}, device_id_type=MESH)

    def a_relay(owner, peer, part):
        piece = flat_ref.at[a_rows(part), a_cols(owner)]
        return pltpu.make_async_remote_copy(
            src_ref=piece, dst_ref=piece,
            send_sem=a_fsem.at[part, owner], recv_sem=a_rsem.at[part, owner],
            device_id={"head": peer}, device_id_type=MESH)

    for step in range(1, n_head):
        w_copy(head, lax.rem(head + step, n_head)).start()
    w_own = pltpu.make_async_copy(
        w_ref.at[:, pl.ds(pl.multiple_of(head * width, 128), width)],
        wbuf.at[pl.ds(pl.multiple_of(head * feat, 128), feat), :], own_sem.at[0])
    w_own.start()

    vall[me] = v_ref[...].T

    ri = lax.broadcasted_iota(jnp.int32, (block, block), 0)
    ci = lax.broadcasted_iota(jnp.int32, (block, block), 1)
    eye = ri == ci
    strict = ri > ci

    scales = []
    for b in range(blocks):
        part = slice(b * block, (b + 1) * block)
        hb = h_ref[part, :]
        gram = lax.dot_general(hb, hb, NT, preferred_element_type=F32)
        diag = jnp.where(eye, gram, 0.0)
        r_col = lax.rsqrt(jnp.sum(diag, axis=1, keepdims=True) + EPSILON)
        r_row = lax.rsqrt(jnp.sum(diag, axis=0, keepdims=True) + EPSILON)
        beta_row = rates_ref[:, part]
        beta_col = jnp.sum(jnp.where(eye, beta_row, 0.0), axis=1, keepdims=True)
        lower = jnp.where(strict, gram * (beta_col * r_col) * r_row, 0.0)
        nmat[b] = lower
        first = jnp.logical_and((ri >> 1) == (ci >> 1), strict)
        inv[b] = jnp.where(eye, 1.0, 0.0) - jnp.where(first, lower, 0.0)
        scales.append((r_col, r_row * beta_row))

    to_later(v_copy, lambda copy: copy.start())

    def level(depth, carry):
        near = jnp.logical_and((ri >> (depth + 1)) == (ci >> (depth + 1)), (ri >> depth) != (ci >> depth))
        xs = [inv[b] for b in range(blocks)]
        parts = [split(x) for x in xs]
        ys = []
        for b in range(blocks):
            (mh, ml), (xh, xl) = split(jnp.where(near, nmat[b], 0.0)), parts[b]
            ys.append(mm(mh, xh) + mm(ml, xh) + mm(mh, xl))
        for b in range(blocks):
            (yh, yl), (xh, xl) = split(ys[b]), parts[b]
            inv[b] = xs[b] - (mm(xh, yh) + mm(xl, yh) + mm(xh, yl))
        return carry

    lax.fori_loop(1, block.bit_length() - 1, level, 0)

    fr = lax.broadcasted_iota(jnp.int32, (feat, feat), 0)
    fc = lax.broadcasted_iota(jnp.int32, (feat, feat), 1)
    unit = jnp.where(fr == fc, 1.0, 0.0).astype(F32)
    rights, passages, finals = [], [], []
    for b in range(blocks):
        part = slice(b * block, (b + 1) * block)
        hb, kb = h_ref[part, :], k_ref[part, :]
        r_col, rb_row = scales[b]
        th, tl = split(inv[b] * r_col * rb_row)
        wk = lax.dot_general(hb, kb, NT, preferred_element_type=F32)
        wh, wl = split(jnp.where(strict, wk, 0.0))
        rk = mm(th, wh) + mm(tl, wh) + mm(th, wl)
        rh = mm(th, hb) + mm(tl, hb)
        hbt = hb.astype(F32).T.astype(BF16)
        rkh, rkl = split(rk)
        rhh, rhl = split(rh)
        finals.append(kb.astype(F32).T - (mm(hbt, rkh) + mm(hbt, rkl)))
        passages.append(unit - (mm(hbt, rhh) + mm(hbt, rhl)))
        rights.append((rkh, rkl, rhh, rhl))

    prefixes = [None]
    now = finals[0]
    prefix = passages[0]
    for b in range(1, blocks):
        moved[b - 1, :, : b * block] = now
        prefixes.append(prefix)
        now = jnp.concatenate([dot3(passages[b], now), finals[b]], 1)
        prefix = dot3(passages[b], prefix)
    kall[me, :rows, :] = now.T.astype(BF16)
    kall[me, rows:, :] = prefix.T.astype(BF16)
    to_later(k_copy, lambda copy: copy.start())

    def pass_values(i, carry):
        source = me - 2 - 2 * i
        v_copy(source, me).wait_recv()
        v_forward(source).start()
        return carry
    lax.fori_loop(0, earlier_pairs, pass_values, 0)

    for b in range(blocks):
        part = slice(b * block, (b + 1) * block)
        hb, kb, qb = h_ref[part, :], k_ref[part, :], q_ref[part, :]
        rkh, rkl, rhh, rhl = rights[b]
        qw = lax.dot_general(qb, hb, NT, preferred_element_type=F32)
        qwh, qwl = split(jnp.where(ri >= ci, qw, 0.0))
        qk = lax.dot_general(qb, kb, NT, preferred_element_type=F32)
        inside = (qk - (mm(qwh, rkh) + mm(qwl, rkh) + mm(qwh, rkl))) * scale
        scores = jnp.where(ri >= ci, inside, NEGATIVE)
        start = (qb.astype(F32) - (mm(qwh, rhh) + mm(qwl, rhh) + mm(qwh, rhl))) * scale
        if b:
            scores = jnp.concatenate([dot3(start, moved[b - 1, :, : b * block]), scores], 1)
            start = dot3(start, prefixes[b])
        mov[:, part] = start.T
        top = jnp.max(scores, axis=1, keepdims=True)
        weight = jnp.exp(scores - top)
        peak[:, part] = jnp.sum(jnp.where(eye, top, 0.0), axis=0, keepdims=True)
        summed = jnp.sum(weight, axis=1, keepdims=True)
        total[:, part] = jnp.sum(jnp.where(eye, summed, 0.0), axis=0, keepdims=True)
        acc[:, part] = mm(weight.astype(BF16), v_ref[: (b + 1) * block, :]).T

    def attend(cols, sources):
        moving = mov[:, cols]
        scores = []
        for source in sources:
            qcat = jnp.concatenate(split(moving), 0)
            keys = kall[source]
            out = mm(jnp.concatenate([keys, keys], 1), qcat)
            scores.append(out[:rows])
            moving = out[rows:]
        mov[:, cols] = moving
        old = peak[:, cols]
        top = old
        for s in scores:
            top = jnp.maximum(top, jnp.max(s, axis=0, keepdims=True))
        shrink = jnp.exp(old - top)
        peak[:, cols] = top
        summed = total[:, cols] * shrink
        gathered = acc[:, cols] * shrink
        for source, s in zip(sources, scores):
            weight = jnp.exp(s - top)
            summed = summed + jnp.sum(weight, axis=0, keepdims=True)
            gathered = gathered + mm(vall[source], weight.astype(BF16))
        total[:, cols] = summed
        acc[:, cols] = gathered

    def relayed(owner, peer):
        if n_head < 3:
            return owner != owner
        return jnp.logical_or(jnp.logical_and(owner == 0, peer == n_head - 1),
                              jnp.logical_and(owner == n_head - 1, peer == 0))

    def direct(part, action):
        for peer in range(n_head):
            @pl.when(jnp.logical_and(head != peer, jnp.logical_not(relayed(head, peer))))
            def _():
                action(a_copy(head, peer, part))

    per_half = span // block
    for part in range(halves):
        @pl.when(odd == 1)
        def _():
            if part == 0:
                k_copy(me - 1, me).wait_recv()
                v_copy(me - 1, me).wait_recv()
            for t in range(per_half):
                attend(pl.ds(part * span + t * block, block), [me - 1])

        def visit(i, carry):
            low = (earlier_pairs - 1 - i) * 2
            if part == 0:
                mine, other = low + odd, low + 1 - odd
                k_copy(mine, me).wait_recv()
                k_forward(mine).start()
                k_copy(other, me).wait_recv()
                v_copy(other, me).wait_recv()
            for t in range(per_half):
                attend(pl.ds(part * span + t * block, block), [low + 1, low])
            return carry

        lax.fori_loop(0, earlier_pairs, visit, 0)
        for t in range(per_half):
            cols = pl.ds(part * span + t * block, block)
            att[cols, :] = (acc[:, cols] / total[:, cols]).T.astype(BF16)
        direct(part, lambda copy: copy.start())
        pltpu.make_async_copy(
            att.at[a_rows(part), :], flat_ref.at[a_rows(part), a_cols(head)], out_sem.at[part]).start()
        if part == 0:
            for step in range(1, n_head):
                other = lax.rem(head + step, n_head)
                w_copy(other, head).wait_recv()
                w_swap(other, odd).start()
            w_own.wait()

    if n_head >= 3:
        for part in range(halves):
            for owner, relay, peer in ((0, n_head - 2, n_head - 1), (n_head - 1, 1, 0)):
                @pl.when(head == relay)
                def _():
                    a_copy(owner, relay, part).wait_recv()
                    a_relay(owner, peer, part).start()

    for step in range(1, n_head):
        w_swap(lax.rem(head + step, n_head), 1 - odd).wait_recv()
    w_out = pltpu.make_async_copy(wbuf, cols_ref, own_sem.at[1])
    w_out.start()

    to_later(v_copy, lambda copy: copy.wait_send())
    to_later(k_copy, lambda copy: copy.wait_send())

    def passed(i, carry):
        source = me - 2 - 2 * i
        v_forward(source).wait_send()
        k_forward(source).wait_send()
        return carry
    lax.fori_loop(0, earlier_pairs, passed, 0)

    for step in range(1, n_head):
        other = lax.rem(head + step, n_head)
        w_copy(head, other).wait_send()
        w_swap(other, odd).wait_send()

    for part in range(halves):
        direct(part, lambda copy: copy.wait_send())
        for owner in range(n_head):
            skip = head != owner
            if n_head >= 3 and owner in (0, n_head - 1):
                relay = n_head - 2 if owner == 0 else 1
                skip = jnp.logical_and(skip, head != relay)

                @pl.when(head == relay)
                def _():
                    a_relay(owner, head, part).wait_send()

            @pl.when(skip)
            def _():
                a_copy(owner, head, part).wait_recv()
        pltpu.make_async_copy(
            att.at[a_rows(part), :], flat_ref.at[a_rows(part), a_cols(head)], out_sem.at[part]).wait()
    w_out.wait()


def project(flat_ref, cols_ref, att_ref, out_ref):
    feat = att_ref.shape[1]

    @pl.when(pl.program_id(0) == 0)
    def _():
        head = lax.axis_index("head")
        att_ref[...] = flat_ref[:, pl.ds(pl.multiple_of(head * feat, 128), feat)]

    out_ref[...] = mm(flat_ref[...], cols_ref[...]).astype(BF16)


def solution(mesh):
    n_ctx, n_head = mesh.shape["ctx"], mesh.shape["head"]

    def body(queries, keys, values, house, rates, out_weight):
        rows, _, feat = queries.shape
        block = min(256, rows)
        blocks = rows // block
        halves = 2 if blocks % 2 == 0 else 1
        width = out_weight.shape[1] // n_head
        vmem = pl.BlockSpec(memory_space=pltpu.VMEM)
        hbm = pl.BlockSpec(memory_space=pl.ANY)
        dma = pltpu.SemaphoreType.DMA
        flat, columns = pl.pallas_call(
            functools.partial(kernel, n_ctx, n_head, block, halves),
            out_shape=(
                jax.ShapeDtypeStruct((rows, n_head * feat), BF16),
                jax.ShapeDtypeStruct((n_head * feat, width), BF16),
            ),
            in_specs=[vmem] * 5 + [hbm],
            out_specs=(hbm, hbm),
            scratch_shapes=[
                pltpu.VMEM((n_ctx, rows + feat, feat), BF16),
                pltpu.VMEM((n_ctx, feat, rows), BF16),
                pltpu.VMEM((n_head * feat, width), BF16),
                pltpu.VMEM((rows, feat), BF16),
                pltpu.VMEM((blocks, block, block), F32),
                pltpu.VMEM((blocks, block, block), F32),
                pltpu.VMEM((max(blocks - 1, 1), feat, rows), F32),
                pltpu.VMEM((feat, rows), F32),
                pltpu.VMEM((feat, rows), F32),
                pltpu.VMEM((1, rows), F32),
                pltpu.VMEM((1, rows), F32),
                dma((n_ctx,)), dma((n_ctx,)), dma((n_ctx,)), dma((n_ctx,)), dma((n_ctx,)), dma((n_ctx,)),
                dma((n_head,)), dma((n_head,)), dma((n_head,)), dma((n_head,)),
                dma((halves, n_head)), dma((halves, n_head)), dma((halves, n_head)), dma((2,)), dma((halves,)),
            ],
            compiler_params=pltpu.CompilerParams(
                collective_id=0, has_side_effects=True, vmem_limit_bytes=60 * 1024 * 1024),
            name="path_attention",
        )(queries.reshape(rows, feat), keys.reshape(rows, feat), values.reshape(rows, feat),
          house.reshape(rows, feat), rates, out_weight)
        tile = min(512, width)
        attended, projected = pl.pallas_call(
            project,
            grid=(width // tile,),
            out_shape=(
                jax.ShapeDtypeStruct((rows, feat), BF16),
                jax.ShapeDtypeStruct((rows, width), BF16),
            ),
            in_specs=[
                pl.BlockSpec((rows, n_head * feat), lambda i: (0, 0)),
                pl.BlockSpec((n_head * feat, tile), lambda i: (0, i)),
            ],
            out_specs=(
                pl.BlockSpec((rows, feat), lambda i: (0, 0)),
                pl.BlockSpec((rows, tile), lambda i: (0, i)),
            ),
            compiler_params=pltpu.CompilerParams(vmem_limit_bytes=40 * 1024 * 1024),
            name="projection",
        )(flat, columns)
        return attended.reshape(rows, 1, feat), projected

    in_specs = (
        P("ctx", "head", None),
        P("ctx", "head", None),
        P("ctx", "head", None),
        P("ctx", "head", None),
        P("head", "ctx"),
        P("head", None),
    )
    out_specs = (P("ctx", "head", None), P("ctx", "head"))
    return jax.shard_map(body, mesh=mesh, in_specs=in_specs, out_specs=out_specs, check_vma=False)
```

```python
import functools

import jax
import jax.numpy as jnp
from jax import lax
from jax.experimental import pallas as pl
from jax.experimental.pallas import tpu as pltpu
from jax.sharding import PartitionSpec as P

EPSILON = 1e-06
NEGATIVE = -1e30
MESH = pl.DeviceIdType.MESH
F32 = jnp.float32
BF16 = jnp.bfloat16
NT = (((1,), (1,)), ((), ()))
LOG2E = 1.4426950408889634


def mm(a, b):
    return jnp.dot(a, b, preferred_element_type=F32)


def split(x):
    high = x.astype(BF16)
    return high, (x - high.astype(F32)).astype(BF16)


def twice(x, axis):
    return jnp.concatenate([x, x], axis)


def mm3(a, b):
    (ah, al), (bh, bl) = a, b
    return mm(jnp.concatenate([ah, al], 1), twice(bh, 0)) + mm(ah, bl)


def kernel(
    n_ctx, n_head, block, tile, halves,
    q_hbm, k_hbm, v_hbm, h_hbm, rates_hbm, w_ref,
    attended_ref, proj_ref,
    q_ref, k_ref, v_ref, h_ref, rates_ref, kall, vall, wbuf, flat_ref, att, near, mov, acc, peak,
    v_ssem, v_fsem, v_rsem, v_lsem, k_ssem, k_fsem, k_rsem, k_lsem,
    w_ssem, w_rsem, wf_ssem, wf_rsem, a_ssem, a_rsem, a_fsem, own_sem, in_sem,
):
    me = lax.axis_index("ctx")
    head = lax.axis_index("head")
    rows, feat = q_ref.shape
    blocks = rows // block
    width = wbuf.shape[1]
    half_width = width // 2
    scale = feat ** (-0.5) * LOG2E
    odd = lax.rem(me, 2)
    partner = me + 1 - 2 * odd
    later_pairs = (n_ctx - 1 - me) // 2
    earlier_pairs = me // 2
    span = rows // halves

    loads = [
        pltpu.make_async_copy(source, target, in_sem.at[i]) for i, (source, target) in enumerate((
            (v_hbm, v_ref), (h_hbm, h_ref), (rates_hbm, rates_ref), (k_hbm, k_ref), (q_hbm, q_ref)))]
    for load in loads:
        load.start()

    barrier = pltpu.get_barrier_semaphore()
    for step in range(1, n_ctx):
        pl.semaphore_signal(barrier, inc=1, device_id={"ctx": lax.rem(me + step, n_ctx)}, device_id_type=MESH)
    for step in range(1, n_head):
        pl.semaphore_signal(barrier, inc=1, device_id={"head": lax.rem(head + step, n_head)}, device_id_type=MESH)
    loads[0].wait()
    vall[me, :feat, :] = v_ref[...].T
    pl.semaphore_wait(barrier, n_ctx + n_head - 2)

    def slab(piece, owner, send, recv, peer):
        return pltpu.make_async_remote_copy(
            src_ref=piece, dst_ref=piece, send_sem=send, recv_sem=recv.at[owner],
            device_id={"ctx": peer}, device_id_type=MESH)

    def v_copy(owner, peer):
        return slab(vall.at[owner, :feat], owner, v_ssem.at[peer], v_rsem, peer)

    def k_copy(owner, peer):
        return slab(kall.at[owner], owner, k_ssem.at[peer], k_rsem, peer)

    def v_forward(owner):
        return slab(vall.at[owner, :feat], owner, v_fsem.at[owner], v_rsem, partner)

    def k_forward(owner):
        return slab(kall.at[owner], owner, k_fsem.at[owner], k_rsem, partner)

    def v_relay(owner, peer):
        return slab(vall.at[owner, :feat], owner, v_lsem.at[owner], v_rsem, peer)

    def k_relay(owner, peer):
        return slab(kall.at[owner], owner, k_lsem.at[owner], k_rsem, peer)

    square = n_ctx == 8
    relays = ((2, 0, 6), (5, 1, 7), (7, 3, 5)) if square else ()

    def to_later(copy, action):
        if square:
            @pl.when(me == 2)
            def _():
                action(copy(me, 4))

            for group, targets in ((0, (1, 2)), (1, (3,)), (2, (3,))):
                @pl.when(me // 2 == group)
                def _():
                    for target in targets:
                        action(copy(me, 2 * target + odd))
        else:
            def go(i, carry):
                action(copy(me, me + 2 * (later_pairs - i)))
                return carry
            lax.fori_loop(0, later_pairs, go, 0)

        @pl.when(odd == 0)
        def _():
            action(copy(me, me + 1))

    def half_cols(base, which):
        return pl.ds(pl.multiple_of(base + which * half_width, 128), half_width)

    def w_copy(owner, peer):
        return pltpu.make_async_remote_copy(
            src_ref=w_ref.at[:, half_cols(peer * width, odd)],
            dst_ref=wbuf.at[pl.ds(pl.multiple_of(owner * feat, 128), feat), half_cols(0, odd)],
            send_sem=w_ssem.at[peer], recv_sem=w_rsem.at[owner],
            device_id={"head": peer}, device_id_type=MESH)

    def w_swap(owner, which):
        part = wbuf.at[pl.ds(pl.multiple_of(owner * feat, 128), feat), half_cols(0, which)]
        return pltpu.make_async_remote_copy(
            src_ref=part, dst_ref=part, send_sem=wf_ssem.at[owner], recv_sem=wf_rsem.at[owner],
            device_id={"ctx": partner}, device_id_type=MESH)

    def a_rows(part):
        return pl.ds(part * span, span)

    def a_cols(owner):
        return pl.ds(pl.multiple_of(owner * feat, 128), feat)

    def a_copy(owner, peer, part):
        return pltpu.make_async_remote_copy(
            src_ref=att.at[a_rows(part), :], dst_ref=flat_ref.at[a_rows(part), a_cols(owner)],
            send_sem=a_ssem.at[part, peer], recv_sem=a_rsem.at[part, owner],
            device_id={"head": peer}, device_id_type=MESH)

    def a_relay(owner, peer, part):
        piece = flat_ref.at[a_rows(part), a_cols(owner)]
        return pltpu.make_async_remote_copy(
            src_ref=piece, dst_ref=piece,
            send_sem=a_fsem.at[part, owner], recv_sem=a_rsem.at[part, owner],
            device_id={"head": peer}, device_id_type=MESH)

    for step in range(1, n_head):
        w_copy(head, lax.rem(head + step, n_head)).start()
    w_own = pltpu.make_async_copy(
        w_ref.at[:, pl.ds(pl.multiple_of(head * width, 128), width)],
        wbuf.at[pl.ds(pl.multiple_of(head * feat, 128), feat), :], own_sem.at[0])
    w_own.start()

    ri = lax.broadcasted_iota(jnp.int32, (block, block), 0)
    ci = lax.broadcasted_iota(jnp.int32, (block, block), 1)
    eye = ri == ci
    unit = jnp.where(eye, 1.0, 0.0).astype(F32)
    strict = ri < ci
    every = range(blocks)
    parts = [slice(b * block, (b + 1) * block) for b in every]

    def within(fine, coarse):
        return jnp.logical_and((ri >> coarse) == (ci >> coarse), (ri >> fine) != (ci >> fine))

    for load in loads[1:4]:
        load.wait()
    ups, khs, steps = [], [], []
    for b in every:
        hb, kb = h_ref[parts[b], :], k_ref[parts[b], :]
        both = lax.dot_general(jnp.concatenate([hb, kb], 0), hb, NT, preferred_element_type=F32)
        gram = both[:block]
        norm = jnp.sum(jnp.where(eye, gram, 0.0), axis=0, keepdims=True) + EPSILON
        step_row = rates_ref[:, parts[b]] / norm
        steps.append(jnp.sum(jnp.where(eye, step_row, 0.0), axis=1, keepdims=True))
        ups.append(jnp.where(strict, gram * step_row, 0.0))
        khs.append(jnp.where(strict, both[block:], 0.0))

    to_later(v_copy, lambda copy: copy.start())
    loads[4].wait()
    vall[:, feat:, :] = jnp.ones((n_ctx, vall.shape[1] - feat, rows), BF16)

    base = [jnp.where(within(0, 3), u, 0.0) for u in ups]
    bs = [split(u) for u in base]
    squares = [mm3(p, p) for p in bs]
    qs = [split(x) for x in squares]
    cubes = [mm3(bs[b], qs[b]) for b in every]
    fourths = [mm3(qs[b], qs[b]) for b in every]
    firsts = [unit - base[b] + squares[b] - cubes[b] for b in every]
    invs = [firsts[b] + mm3(split(firsts[b]), split(fourths[b])) for b in every]
    size = 3
    while (1 << size) < block:
        top = min(size + 2, block.bit_length() - 1)
        xs = [split(x) for x in invs]
        offs = [split(jnp.where(within(size, top), u, 0.0)) for u in ups]
        zs = [split(mm3(xs[b], offs[b])) for b in every]
        ones = [invs[b] - mm3(zs[b], xs[b]) for b in every]
        if top == size + 2:
            twos = [split(mm3(zs[b], zs[b])) for b in every]
            ones = [ones[b] + mm3(twos[b], split(ones[b])) for b in every]
        invs = ones
        size = top

    for device, owner, peer in relays:
        @pl.when(me == device)
        def _():
            v_copy(owner, me).wait_recv()
            v_relay(owner, peer).start()

    rights, groups = [], []
    for b in every:
        hb, kb = h_ref[parts[b], :], k_ref[parts[b], :]
        th, tl = split(invs[b] * steps[b])
        kh, kl = split(khs[b])
        left = jnp.concatenate([kh, hb.T], 0)
        right = mm(twice(left, 1), jnp.concatenate([th, tl], 0))
        right = jnp.concatenate([right[:block] + mm(kl, th), right[block:]], 0)
        rh, rl = split(right)
        rights.append((rh, jnp.concatenate([rh, rl], 1)))
        change = mm(rights[b][1], twice(hb, 0))
        groups.append((kb.astype(F32) - change[:block], unit - change[block:]))

    levels = []
    while len(groups) > 1:
        merged, level = [], []
        for g in range(0, len(groups) - 1, 2):
            (early, early_all), (late, late_all) = groups[g], groups[g + 1]
            joined = jnp.concatenate([early, early_all], 0)
            parted = split(joined)
            level.append(parted[0])
            out = mm3(parted, split(late_all))
            merged.append((jnp.concatenate([out[:-feat], late], 0), out[-feat:]))
        levels.append(level)
        groups = merged
    kall[me, :rows, :] = groups[0][0].astype(BF16)
    kall[me, rows:, :] = groups[0][1].astype(BF16)
    to_later(k_copy, lambda copy: copy.start())

    def pass_values(i, carry):
        source = me - 2 - 2 * i
        taken = source < 0
        for device, owner, _ in relays:
            taken = jnp.logical_or(taken, jnp.logical_and(me == device, source == owner))

        @pl.when(jnp.logical_not(taken))
        def _():
            v_copy(source, me).wait_recv()
        v_forward(source).start()
        return carry
    lax.fori_loop(0, earlier_pairs, pass_values, 0)

    moving = []
    for b in every:
        hb, kb, qb = h_ref[parts[b], :], k_ref[parts[b], :], q_ref[parts[b], :]
        both = lax.dot_general(jnp.concatenate([hb, kb], 0), qb, NT, preferred_element_type=F32)
        wh, wl = split(jnp.where(ri <= ci, both[:block], 0.0))
        change = mm(rights[b][1], twice(wh, 0)) + mm(rights[b][0], wl)
        inside = (both[block:] - change[:block]) * scale
        near[parts[b], parts[b]] = jnp.where(ri <= ci, inside, NEGATIVE)
        moving.append((qb.T.astype(F32) - change[block:]) * scale)
    width_now = block
    for level in levels:
        joined = []
        for g, keys in enumerate(level):
            first = 2 * g * width_now
            out = mm(twice(keys, 1), jnp.concatenate(split(moving[2 * g + 1]), 0))
            near[first : first + width_now, first + width_now : first + 2 * width_now] = out[:-feat]
            near[first + width_now : first + 2 * width_now, first : first + width_now] = jnp.full(
                (width_now, width_now), NEGATIVE, F32)
            joined.append(jnp.concatenate([moving[2 * g], out[-feat:]], 1))
        moving = joined
        width_now *= 2
    mov[...] = moving[0]
    for t in range(rows // tile):
        cols = slice(t * tile, (t + 1) * tile)
        seen = (t + 1) * tile
        scores = near[:seen, cols]
        top = jnp.max(scores, axis=0, keepdims=True)
        peak[:, cols] = top
        acc[:, cols] = mm(vall[me, :, :seen], jnp.exp2(scores - top).astype(BF16))

    def attend(tiles, sources):
        every_score = []
        for cols in tiles:
            current = mov[:, cols]
            scores = []
            for source in sources:
                out = mm(twice(kall[source], 1), jnp.concatenate(split(current), 0))
                scores.append(out[:rows])
                current = out[rows:]
            mov[:, cols] = current
            every_score.append(scores)
        for cols, scores in zip(tiles, every_score):
            old = peak[:, cols]
            top = old
            for s in scores:
                top = jnp.maximum(top, jnp.max(s, axis=0, keepdims=True))
            peak[:, cols] = top
            gathered = acc[:, cols] * jnp.exp2(old - top)
            for source, s in zip(sources, scores):
                gathered = gathered + mm(vall[source], jnp.exp2(s - top).astype(BF16))
            acc[:, cols] = gathered

    def relayed(owner, peer):
        if n_head < 3:
            return owner != owner
        return jnp.logical_or(jnp.logical_and(owner == 0, peer == n_head - 1),
                              jnp.logical_and(owner == n_head - 1, peer == 0))

    def direct(part, action):
        for peer in range(n_head):
            @pl.when(jnp.logical_and(head != peer, jnp.logical_not(relayed(head, peer))))
            def _():
                action(a_copy(head, peer, part))

    groups_of = [[pl.ds(part * span + t * tile, tile) for t in range(span // tile)] for part in range(halves)]
    for device, owner, peer in relays:
        @pl.when(me == device)
        def _():
            k_copy(owner, me).wait_recv()
            k_relay(owner, peer).start()
            k_forward(owner).start()

    for part in range(halves):
        @pl.when(odd == 1)
        def _():
            if part == 0:
                k_copy(me - 1, me).wait_recv()
                v_copy(me - 1, me).wait_recv()
            attend(groups_of[part], [me - 1])

        def visit(i, carry):
            low = (earlier_pairs - 1 - i) * 2
            if part == 0:
                mine, other = low + odd, low + 1 - odd
                taken = mine < 0
                for device, owner, _ in relays:
                    taken = jnp.logical_or(taken, jnp.logical_and(me == device, mine == owner))

                @pl.when(jnp.logical_not(taken))
                def _():
                    k_copy(mine, me).wait_recv()
                    k_forward(mine).start()
                k_copy(other, me).wait_recv()
                v_copy(other, me).wait_recv()
            attend(groups_of[part], [low + 1, low])
            return carry

        lax.fori_loop(0, earlier_pairs, visit, 0)
        for cols in groups_of[part]:
            att[cols, :] = (acc[:feat, cols] / acc[feat : feat + 1, cols]).T.astype(BF16)
        direct(part, lambda copy: copy.start())
        attended_ref[a_rows(part), :] = att[a_rows(part), :]
        flat_ref[a_rows(part), a_cols(head)] = att[a_rows(part), :]
        if part == 0:
            for step in range(1, n_head):
                other = lax.rem(head + step, n_head)
                w_copy(other, head).wait_recv()
                w_swap(other, odd).start()
            w_own.wait()

    for step in range(1, n_head):
        w_swap(lax.rem(head + step, n_head), 1 - odd).wait_recv()

    to_later(v_copy, lambda copy: copy.wait_send())
    to_later(k_copy, lambda copy: copy.wait_send())

    def passed(i, carry):
        source = me - 2 - 2 * i
        v_forward(source).wait_send()
        k_forward(source).wait_send()
        return carry
    lax.fori_loop(0, earlier_pairs, passed, 0)
    for device, owner, peer in relays:
        @pl.when(me == device)
        def _():
            v_relay(owner, peer).wait_send()
            k_relay(owner, peer).wait_send()

    for step in range(1, n_head):
        other = lax.rem(head + step, n_head)
        w_copy(head, other).wait_send()
        w_swap(other, odd).wait_send()

    for part in range(halves):
        if n_head >= 3:
            for owner, relay, peer in ((0, n_head - 2, n_head - 1), (n_head - 1, 1, 0)):
                @pl.when(head == relay)
                def _():
                    a_copy(owner, relay, part).wait_recv()
                    a_relay(owner, peer, part).start()
        for owner in range(n_head):
            skip = head != owner
            if n_head >= 3 and owner in (0, n_head - 1):
                skip = jnp.logical_and(skip, head != (n_head - 2 if owner == 0 else 1))

            @pl.when(skip)
            def _():
                a_copy(owner, head, part).wait_recv()

        def project(i, carry):
            out_rows = pl.ds(pl.multiple_of(part * span + (i // strips) * tall, tall), tall)
            out_cols = pl.ds(pl.multiple_of(lax.rem(i, strips) * wide, 128), wide)
            proj_ref[out_rows, out_cols] = mm(flat_ref[out_rows, :], wbuf[:, out_cols]).astype(BF16)
            return carry

        tall, wide = min(256, span), min(512, width)
        strips = width // wide
        lax.fori_loop(0, (span // tall) * strips, project, 0)

    for part in range(halves):
        direct(part, lambda copy: copy.wait_send())
        if n_head >= 3:
            for owner, relay, peer in ((0, n_head - 2, n_head - 1), (n_head - 1, 1, 0)):
                @pl.when(head == relay)
                def _():
                    a_relay(owner, peer, part).wait_send()


def solution(mesh):
    n_ctx, n_head = mesh.shape["ctx"], mesh.shape["head"]

    def body(queries, keys, values, house, rates, out_weight):
        rows, _, feat = queries.shape
        block = feat
        tile = min(256, rows)
        halves = 2 if rows % (2 * tile) == 0 else 1
        width = out_weight.shape[1] // n_head
        vmem = pl.BlockSpec(memory_space=pltpu.VMEM)
        hbm = pl.BlockSpec(memory_space=pltpu.HBM)
        dma = pltpu.SemaphoreType.DMA
        attended, projected = pl.pallas_call(
            functools.partial(kernel, n_ctx, n_head, block, tile, halves),
            out_shape=(
                pltpu.VMEM((rows, feat), BF16),
                pltpu.VMEM((rows, width), BF16),
            ),
            in_specs=[hbm] * 6,
            out_specs=(vmem, vmem),
            scratch_shapes=[pltpu.VMEM((rows, feat), BF16)] * 4 + [
                pltpu.VMEM((1, rows), F32),
                pltpu.VMEM((n_ctx, rows + feat, feat), BF16),
                pltpu.VMEM((n_ctx, feat + 16, rows), BF16),
                pltpu.VMEM((n_head * feat, width), BF16),
                pltpu.VMEM((rows, n_head * feat), BF16),
                pltpu.VMEM((rows, feat), BF16),
                pltpu.VMEM((rows, rows), F32),
                pltpu.VMEM((feat, rows), F32),
                pltpu.VMEM((feat + 16, rows), F32),
                pltpu.VMEM((1, rows), F32),
                dma((n_ctx,)), dma((n_ctx,)), dma((n_ctx,)), dma((n_ctx,)), dma((n_ctx,)), dma((n_ctx,)), dma((n_ctx,)), dma((n_ctx,)),
                dma((n_head,)), dma((n_head,)), dma((n_head,)), dma((n_head,)),
                dma((halves, n_head)), dma((halves, n_head)), dma((halves, n_head)), dma((1,)), dma((5,)),
            ],
            compiler_params=pltpu.CompilerParams(
                collective_id=0, has_side_effects=True, vmem_limit_bytes=66 * 1000 * 1000 - 2 * rows * (width + feat)),
            name="path_attention",
        )(queries.reshape(rows, feat), keys.reshape(rows, feat), values.reshape(rows, feat),
          house.reshape(rows, feat), rates, out_weight)
        return attended.reshape(rows, 1, feat), projected

    in_specs = (
        P("ctx", "head", None),
        P("ctx", "head", None),
        P("ctx", "head", None),
        P("ctx", "head", None),
        P("head", "ctx"),
        P("head", None),
    )
    out_specs = (P("ctx", "head", None), P("ctx", "head"))
    return jax.shard_map(body, mesh=mesh, in_specs=in_specs, out_specs=out_specs, check_vma=False)
```

```python
import functools

import jax
import jax.numpy as jnp
from jax import lax
from jax.experimental import pallas as pl
from jax.experimental.pallas import tpu as pltpu
from jax.sharding import PartitionSpec as P

EPSILON = 1e-06
NEGATIVE = -1e30
MESH = pl.DeviceIdType.MESH
F32 = jnp.float32
BF16 = jnp.bfloat16
NT = (((1,), (1,)), ((), ()))
LOG2E = 1.4426950408889634


def mm(a, b):
    return jnp.dot(a, b, preferred_element_type=F32)


def split(x):
    high = x.astype(BF16)
    return high, (x - high.astype(F32)).astype(BF16)


def twice(x, axis):
    return jnp.concatenate([x, x], axis)


def mm3(a, b):
    (ah, al), (bh, bl) = a, b
    return mm(jnp.concatenate([ah, al], 1), twice(bh, 0)) + mm(ah, bl)


def kernel(
    n_ctx, n_head, block, tile, halves,
    q_hbm, k_hbm, v_hbm, h_hbm, rates_hbm, w_ref,
    attended_ref, proj_ref,
    q_ref, k_ref, v_ref, h_ref, rates_ref, kall, vall, wbuf, flat_ref, att, near, mov, acc, peak,
    v_ssem, v_fsem, v_rsem, v_lsem, k_ssem, k_fsem, k_rsem, k_lsem,
    w_ssem, w_rsem, wf_ssem, wf_rsem, a_ssem, a_rsem, a_fsem, own_sem, in_sem,
):
    me = lax.axis_index("ctx")
    head = lax.axis_index("head")
    rows, feat = q_ref.shape
    blocks = rows // block
    width = wbuf.shape[1]
    share = 4 if n_ctx % 4 == 0 else 2
    quarter = width // share
    mine_q = lax.rem(me, share)
    across = me + 2 - 4 * (lax.rem(me, 4) // 2)
    scale = feat ** (-0.5) * LOG2E
    odd = lax.rem(me, 2)
    partner = me + 1 - 2 * odd
    later_pairs = (n_ctx - 1 - me) // 2
    earlier_pairs = me // 2
    span = rows // halves

    loads = [
        pltpu.make_async_copy(source, target, in_sem.at[i]) for i, (source, target) in enumerate((
            (v_hbm, v_ref), (h_hbm, h_ref), (rates_hbm, rates_ref), (k_hbm, k_ref), (q_hbm, q_ref)))]
    for load in loads:
        load.start()

    barrier = pltpu.get_barrier_semaphore()
    for step in range(1, n_ctx):
        pl.semaphore_signal(barrier, inc=1, device_id={"ctx": lax.rem(me + step, n_ctx)}, device_id_type=MESH)
    for step in range(1, n_head):
        pl.semaphore_signal(barrier, inc=1, device_id={"head": lax.rem(head + step, n_head)}, device_id_type=MESH)
    loads[0].wait()
    vall[me, :feat, :] = v_ref[...].T
    pl.semaphore_wait(barrier, n_ctx + n_head - 2)

    def slab(piece, owner, send, recv, peer):
        return pltpu.make_async_remote_copy(
            src_ref=piece, dst_ref=piece, send_sem=send, recv_sem=recv.at[owner],
            device_id={"ctx": peer}, device_id_type=MESH)

    def v_copy(owner, peer):
        return slab(vall.at[owner, :feat], owner, v_ssem.at[peer], v_rsem, peer)

    def k_copy(owner, peer):
        return slab(kall.at[owner], owner, k_ssem.at[peer], k_rsem, peer)

    def v_forward(owner):
        return slab(vall.at[owner, :feat], owner, v_fsem.at[owner], v_rsem, partner)

    def k_forward(owner):
        return slab(kall.at[owner], owner, k_fsem.at[owner], k_rsem, partner)

    def v_relay(owner, peer):
        return slab(vall.at[owner, :feat], owner, v_lsem.at[owner], v_rsem, peer)

    def k_relay(owner, peer):
        return slab(kall.at[owner], owner, k_lsem.at[owner], k_rsem, peer)

    square = n_ctx == 8
    v_relays = ((2, 0, 6), (5, 1, 7), (6, 2, 4), (7, 3, 5)) if square else ()
    k_relays = ((2, 0, 6), (5, 1, 7), (7, 3, 5)) if square else ()

    def to_later(copy, action, whole=True):
        if square:
            if not whole:
                @pl.when(me == 2)
                def _():
                    action(copy(me, 4))

            for group, targets in ((0, (1, 2)), (1, (3,)), (2, (3,))):
                @pl.when(me // 2 == group)
                def _():
                    for target in targets:
                        action(copy(me, 2 * target + odd))
        else:
            def go(i, carry):
                action(copy(me, me + 2 * (later_pairs - i)))
                return carry
            lax.fori_loop(0, later_pairs, go, 0)

        @pl.when(odd == 0)
        def _():
            action(copy(me, me + 1))

    def quarter_cols(base, which):
        return pl.ds(pl.multiple_of(base + which * quarter, 128), quarter)

    def w_piece(owner, which):
        return wbuf.at[pl.ds(pl.multiple_of(owner * feat, 128), feat), quarter_cols(0, which)]

    def w_copy(owner, peer):
        return pltpu.make_async_remote_copy(
            src_ref=w_ref.at[:, quarter_cols(peer * width, mine_q)], dst_ref=w_piece(owner, mine_q),
            send_sem=w_ssem.at[peer], recv_sem=w_rsem.at[owner],
            device_id={"head": peer}, device_id_type=MESH)

    def w_hand(owner, which, way, peer):
        return pltpu.make_async_remote_copy(
            src_ref=w_piece(owner, which), dst_ref=w_piece(owner, which),
            send_sem=wf_ssem.at[way, owner], recv_sem=wf_rsem.at[way, owner],
            device_id={"ctx": peer}, device_id_type=MESH)

    beside = mine_q + 1 - 2 * odd
    over = lax.rem(mine_q + 2, share)
    over_beside = lax.rem(beside + 2, share)

    def a_rows(part):
        return pl.ds(part * span, span)

    def a_cols(owner):
        return pl.ds(pl.multiple_of(owner * feat, 128), feat)

    def a_copy(owner, peer, part):
        return pltpu.make_async_remote_copy(
            src_ref=att.at[a_rows(part), :], dst_ref=flat_ref.at[a_rows(part), a_cols(owner)],
            send_sem=a_ssem.at[part, peer], recv_sem=a_rsem.at[part, owner],
            device_id={"head": peer}, device_id_type=MESH)

    def a_relay(owner, peer, part):
        piece = flat_ref.at[a_rows(part), a_cols(owner)]
        return pltpu.make_async_remote_copy(
            src_ref=piece, dst_ref=piece,
            send_sem=a_fsem.at[part, owner], recv_sem=a_rsem.at[part, owner],
            device_id={"head": peer}, device_id_type=MESH)

    for step in range(1, n_head):
        w_copy(head, lax.rem(head + step, n_head)).start()
    w_own = pltpu.make_async_copy(
        w_ref.at[:, pl.ds(pl.multiple_of(head * width, 128), width)],
        wbuf.at[pl.ds(pl.multiple_of(head * feat, 128), feat), :], own_sem.at[0])
    w_own.start()

    ri = lax.broadcasted_iota(jnp.int32, (block, block), 0)
    ci = lax.broadcasted_iota(jnp.int32, (block, block), 1)
    eye = ri == ci
    unit = jnp.where(eye, 1.0, 0.0).astype(F32)
    strict = ri < ci
    every = range(blocks)
    parts = [slice(b * block, (b + 1) * block) for b in every]

    def within(fine, coarse):
        return jnp.logical_and((ri >> coarse) == (ci >> coarse), (ri >> fine) != (ci >> fine))

    for load in loads[1:4]:
        load.wait()
    ups, khs, steps = [], [], []
    for b in every:
        hb, kb = h_ref[parts[b], :], k_ref[parts[b], :]
        both = lax.dot_general(jnp.concatenate([hb, kb], 0), hb, NT, preferred_element_type=F32)
        gram = both[:block]
        norm = jnp.sum(jnp.where(eye, gram, 0.0), axis=0, keepdims=True) + EPSILON
        step_row = rates_ref[:, parts[b]] / norm
        steps.append(jnp.sum(jnp.where(eye, step_row, 0.0), axis=1, keepdims=True))
        ups.append(jnp.where(strict, gram * step_row, 0.0))
        khs.append(jnp.where(strict, both[block:], 0.0))

    to_later(v_copy, lambda copy: copy.start(), True)
    loads[4].wait()
    vall[:, feat:, :] = jnp.ones((n_ctx, vall.shape[1] - feat, rows), BF16)

    base = [jnp.where(within(0, 3), u, 0.0) for u in ups]
    bs = [split(u) for u in base]
    squares = [mm3(p, p) for p in bs]
    qs = [split(x) for x in squares]
    cubes = [mm3(bs[b], qs[b]) for b in every]
    fourths = [mm3(qs[b], qs[b]) for b in every]
    firsts = [unit - base[b] + squares[b] - cubes[b] for b in every]
    invs = [firsts[b] + mm3(split(firsts[b]), split(fourths[b])) for b in every]
    size = 3
    while (1 << size) < block:
        top = min(size + 2, block.bit_length() - 1)
        xs = [split(x) for x in invs]
        offs = [split(jnp.where(within(size, top), u, 0.0)) for u in ups]
        zs = [split(mm3(xs[b], offs[b])) for b in every]
        ones = [invs[b] - mm3(zs[b], xs[b]) for b in every]
        if top == size + 2:
            twos = [split(mm3(zs[b], zs[b])) for b in every]
            ones = [ones[b] + mm3(twos[b], split(ones[b])) for b in every]
        invs = ones
        size = top

    for device, owner, peer in v_relays:
        @pl.when(me == device)
        def _():
            v_copy(owner, me).wait_recv()
            v_relay(owner, peer).start()

    rights, groups = [], []
    for b in every:
        hb, kb = h_ref[parts[b], :], k_ref[parts[b], :]
        th, tl = split(invs[b] * steps[b])
        kh, kl = split(khs[b])
        left = jnp.concatenate([kh, hb.T], 0)
        right = mm(twice(left, 1), jnp.concatenate([th, tl], 0))
        right = jnp.concatenate([right[:block] + mm(kl, th), right[block:]], 0)
        rh, rl = split(right)
        rights.append((rh, jnp.concatenate([rh, rl], 1)))
        change = mm(rights[b][1], twice(hb, 0))
        groups.append((kb.astype(F32) - change[:block], unit - change[block:]))

    levels = []
    while len(groups) > 1:
        merged, level = [], []
        for g in range(0, len(groups) - 1, 2):
            (early, early_all), (late, late_all) = groups[g], groups[g + 1]
            joined = jnp.concatenate([early, early_all], 0)
            parted = split(joined)
            level.append(parted[0])
            out = mm3(parted, split(late_all))
            merged.append((jnp.concatenate([out[:-feat], late], 0), out[-feat:]))
        levels.append(level)
        groups = merged
    kall[me, :rows, :] = groups[0][0].astype(BF16)
    kall[me, rows:, :] = groups[0][1].astype(BF16)
    to_later(k_copy, lambda copy: copy.start(), False)

    moving = []
    for b in every:
        hb, kb, qb = h_ref[parts[b], :], k_ref[parts[b], :], q_ref[parts[b], :]
        both = lax.dot_general(jnp.concatenate([hb, kb], 0), qb, NT, preferred_element_type=F32)
        wh, wl = split(jnp.where(ri <= ci, both[:block], 0.0))
        change = mm(rights[b][1], twice(wh, 0)) + mm(rights[b][0], wl)
        inside = (both[block:] - change[:block]) * scale
        near[parts[b], parts[b]] = jnp.where(ri <= ci, inside, NEGATIVE)
        moving.append((qb.T.astype(F32) - change[block:]) * scale)
    width_now = block
    for level in levels:
        joined = []
        for g, keys in enumerate(level):
            first = 2 * g * width_now
            out = mm(twice(keys, 1), jnp.concatenate(split(moving[2 * g + 1]), 0))
            near[first : first + width_now, first + width_now : first + 2 * width_now] = out[:-feat]
            near[first + width_now : first + 2 * width_now, first : first + width_now] = jnp.full(
                (width_now, width_now), NEGATIVE, F32)
            joined.append(jnp.concatenate([moving[2 * g], out[-feat:]], 1))
        moving = joined
        width_now *= 2
    mov[...] = moving[0]
    for t in range(rows // tile):
        cols = slice(t * tile, (t + 1) * tile)
        seen = (t + 1) * tile
        scores = near[:seen, cols]
        top = jnp.max(scores, axis=0, keepdims=True)
        peak[:, cols] = top
        acc[:, cols] = mm(vall[me, :, :seen], jnp.exp2(scores - top).astype(BF16))

    def attend(tiles, sources):
        every_score = []
        for cols in tiles:
            current = mov[:, cols]
            scores = []
            for source in sources:
                out = mm(twice(kall[source], 1), jnp.concatenate(split(current), 0))
                scores.append(out[:rows])
                current = out[rows:]
            mov[:, cols] = current
            every_score.append(scores)
        for cols, scores in zip(tiles, every_score):
            old = peak[:, cols]
            top = old
            for s in scores:
                top = jnp.maximum(top, jnp.max(s, axis=0, keepdims=True))
            peak[:, cols] = top
            gathered = acc[:, cols] * jnp.exp2(old - top)
            for source, s in zip(sources, scores):
                gathered = gathered + mm(vall[source], jnp.exp2(s - top).astype(BF16))
            acc[:, cols] = gathered

    def pass_values(i, carry):
        source = me - 2 - 2 * i
        taken = source < 0
        for device, owner, _ in v_relays:
            taken = jnp.logical_or(taken, jnp.logical_and(me == device, source == owner))

        @pl.when(jnp.logical_not(taken))
        def _():
            v_copy(source, me).wait_recv()
        v_forward(source).start()
        return carry
    lax.fori_loop(0, earlier_pairs, pass_values, 0)

    def relayed(owner, peer):
        if n_head < 3:
            return owner != owner
        return jnp.logical_or(jnp.logical_and(owner == 0, peer == n_head - 1),
                              jnp.logical_and(owner == n_head - 1, peer == 0))

    def direct(part, action):
        for beyond, peers in ((True, range(n_head - 1, 0, -1)), (False, range(n_head - 1))):
            for peer in peers:
                wanted = head < peer if beyond else head > peer

                @pl.when(jnp.logical_and(wanted, jnp.logical_not(relayed(head, peer))))
                def _():
                    action(a_copy(head, peer, part))

    groups_of = [[pl.ds(part * span + t * tile, tile) for t in range(span // tile)] for part in range(halves)]
    for device, owner, peer in k_relays:
        @pl.when(me == device)
        def _():
            k_copy(owner, me).wait_recv()
            k_relay(owner, peer).start()
            k_forward(owner).start()

    for part in range(halves):
        @pl.when(odd == 1)
        def _():
            if part == 0:
                k_copy(me - 1, me).wait_recv()
                v_copy(me - 1, me).wait_recv()
            attend(groups_of[part], [me - 1])

        def visit(i, carry):
            low = (earlier_pairs - 1 - i) * 2
            if part == 0:
                mine, other = low + odd, low + 1 - odd
                taken = mine < 0
                for device, owner, _ in k_relays:
                    taken = jnp.logical_or(taken, jnp.logical_and(me == device, mine == owner))

                @pl.when(jnp.logical_not(taken))
                def _():
                    k_copy(mine, me).wait_recv()
                    k_forward(mine).start()
                k_copy(other, me).wait_recv()
                v_copy(other, me).wait_recv()
            attend(groups_of[part], [low + 1, low])
            return carry

        lax.fori_loop(0, earlier_pairs, visit, 0)
        for cols in groups_of[part]:
            att[cols, :] = (acc[:feat, cols] / acc[feat : feat + 1, cols]).T.astype(BF16)
        direct(part, lambda copy: copy.start())
        attended_ref[a_rows(part), :] = att[a_rows(part), :]
        flat_ref[a_rows(part), a_cols(head)] = att[a_rows(part), :]
        if part == 0:
            for step in range(1, n_head):
                other = lax.rem(head + step, n_head)
                w_copy(other, head).wait_recv()
                w_hand(other, mine_q, 0, partner).start()
                if share == 4:
                    w_hand(other, mine_q, 1, across).start()
            w_own.wait()

    others = [lax.rem(head + step, n_head) for step in range(1, n_head)]
    if share == 4:
        for other in others:
            w_hand(other, over, 1, across).wait_recv()
            w_hand(other, over, 2, partner).start()
        for other in others:
            w_hand(other, over_beside, 2, partner).wait_recv()
    for other in others:
        w_hand(other, beside, 0, partner).wait_recv()

    to_later(v_copy, lambda copy: copy.wait_send(), True)
    to_later(k_copy, lambda copy: copy.wait_send(), False)

    def passed(i, carry):
        source = me - 2 - 2 * i
        v_forward(source).wait_send()
        k_forward(source).wait_send()
        return carry
    lax.fori_loop(0, earlier_pairs, passed, 0)
    for relays, relay_copy in ((v_relays, v_relay), (k_relays, k_relay)):
        for device, owner, peer in relays:
            @pl.when(me == device)
            def _():
                relay_copy(owner, peer).wait_send()

    for step in range(1, n_head):
        other = lax.rem(head + step, n_head)
        w_copy(head, other).wait_send()
        w_hand(other, mine_q, 0, partner).wait_send()
        if share == 4:
            w_hand(other, mine_q, 1, across).wait_send()
            w_hand(other, over, 2, partner).wait_send()

    for part in range(halves):
        if n_head >= 3:
            for owner, relay, peer in ((0, n_head - 2, n_head - 1), (n_head - 1, 1, 0)):
                @pl.when(head == relay)
                def _():
                    a_copy(owner, relay, part).wait_recv()
                    a_relay(owner, peer, part).start()
        for owner in range(n_head):
            skip = head != owner
            if n_head >= 3 and owner in (0, n_head - 1):
                skip = jnp.logical_and(skip, head != (n_head - 2 if owner == 0 else 1))

            @pl.when(skip)
            def _():
                a_copy(owner, head, part).wait_recv()

        def project(i, carry):
            out_rows = pl.ds(pl.multiple_of(part * span + (i // strips) * tall, tall), tall)
            out_cols = pl.ds(pl.multiple_of(lax.rem(i, strips) * wide, 128), wide)
            proj_ref[out_rows, out_cols] = mm(flat_ref[out_rows, :], wbuf[:, out_cols]).astype(BF16)
            return carry

        tall, wide = min(256, span), min(512, width)
        strips = width // wide
        lax.fori_loop(0, (span // tall) * strips, project, 0)

    for part in range(halves):
        direct(part, lambda copy: copy.wait_send())
        if n_head >= 3:
            for owner, relay, peer in ((0, n_head - 2, n_head - 1), (n_head - 1, 1, 0)):
                @pl.when(head == relay)
                def _():
                    a_relay(owner, peer, part).wait_send()


def solution(mesh):
    n_ctx, n_head = mesh.shape["ctx"], mesh.shape["head"]

    def body(queries, keys, values, house, rates, out_weight):
        rows, _, feat = queries.shape
        block = feat
        tile = min(256, rows)
        halves = 2 if rows % (2 * tile) == 0 else 1
        width = out_weight.shape[1] // n_head
        vmem = pl.BlockSpec(memory_space=pltpu.VMEM)
        hbm = pl.BlockSpec(memory_space=pltpu.HBM)
        dma = pltpu.SemaphoreType.DMA
        attended, projected = pl.pallas_call(
            functools.partial(kernel, n_ctx, n_head, block, tile, halves),
            out_shape=(
                pltpu.VMEM((rows, feat), BF16),
                pltpu.VMEM((rows, width), BF16),
            ),
            in_specs=[hbm] * 6,
            out_specs=(vmem, vmem),
            scratch_shapes=[pltpu.VMEM((rows, feat), BF16)] * 4 + [
                pltpu.VMEM((1, rows), F32),
                pltpu.VMEM((n_ctx, rows + feat, feat), BF16),
                pltpu.VMEM((n_ctx, feat + 16, rows), BF16),
                pltpu.VMEM((n_head * feat, width), BF16),
                pltpu.VMEM((rows, n_head * feat), BF16),
                pltpu.VMEM((rows, feat), BF16),
                pltpu.VMEM((rows, rows), F32),
                pltpu.VMEM((feat, rows), F32),
                pltpu.VMEM((feat + 16, rows), F32),
                pltpu.VMEM((1, rows), F32),
                dma((n_ctx,)), dma((n_ctx,)), dma((n_ctx,)), dma((n_ctx,)), dma((n_ctx,)), dma((n_ctx,)), dma((n_ctx,)), dma((n_ctx,)),
                dma((n_head,)), dma((n_head,)), dma((3, n_head)), dma((3, n_head)),
                dma((halves, n_head)), dma((halves, n_head)), dma((halves, n_head)), dma((1,)), dma((5,)),
            ],
            compiler_params=pltpu.CompilerParams(
                collective_id=0, has_side_effects=True, vmem_limit_bytes=66 * 1000 * 1000 - 2 * rows * (width + feat)),
            name="path_attention",
        )(queries.reshape(rows, feat), keys.reshape(rows, feat), values.reshape(rows, feat),
          house.reshape(rows, feat), rates, out_weight)
        return attended.reshape(rows, 1, feat), projected

    in_specs = (
        P("ctx", "head", None),
        P("ctx", "head", None),
        P("ctx", "head", None),
        P("ctx", "head", None),
        P("head", "ctx"),
        P("head", None),
    )
    out_specs = (P("ctx", "head", None), P("ctx", "head"))
    return jax.shard_map(body, mesh=mesh, in_specs=in_specs, out_specs=out_specs, check_vma=False)
```

```python
import functools

import jax
import jax.numpy as jnp
from jax import lax
from jax.experimental import pallas as pl
from jax.experimental.pallas import tpu as pltpu
from jax.sharding import PartitionSpec as P

EPSILON = 1e-06
NEGATIVE = -1e30
MESH = pl.DeviceIdType.MESH
F32 = jnp.float32
BF16 = jnp.bfloat16
NT = (((1,), (1,)), ((), ()))
LOG2E = 1.4426950408889634


def mm(a, b):
    return jnp.dot(a, b, preferred_element_type=F32)


def split(x):
    high = x.astype(BF16)
    return high, (x - high.astype(F32)).astype(BF16)


def twice(x, axis):
    return jnp.concatenate([x, x], axis)


def mm3(a, b):
    (ah, al), (bh, bl) = a, b
    return mm(jnp.concatenate([ah, al], 1), twice(bh, 0)) + mm(ah, bl)


def kernel(
    n_ctx, n_head, block, tile, halves,
    q_hbm, k_hbm, v_hbm, h_hbm, rates_hbm, w_ref,
    attended_ref, proj_ref,
    q_ref, k_ref, v_ref, h_ref, rates_ref, kall, vall, wbuf, flat_ref, att, near, mov, acc, peak,
    v_ssem, v_fsem, v_rsem, v_lsem, k_ssem, k_fsem, k_rsem, k_lsem,
    w_ssem, w_rsem, wf_ssem, wf_rsem, a_ssem, a_rsem, a_fsem, own_sem, in_sem,
):
    me = lax.axis_index("ctx")
    head = lax.axis_index("head")
    rows, feat = q_ref.shape
    blocks = rows // block
    width = wbuf.shape[1]
    share = 4 if n_ctx % 4 == 0 else 2
    quarter = width // share
    mine_q = lax.rem(me, share)
    across = me + 2 - 4 * (lax.rem(me, 4) // 2)
    scale = feat ** (-0.5) * LOG2E
    odd = lax.rem(me, 2)
    partner = me + 1 - 2 * odd
    later_pairs = (n_ctx - 1 - me) // 2
    earlier_pairs = me // 2
    span = rows // halves
    pieces = 2 * halves
    strip = rows // pieces

    loads = [
        pltpu.make_async_copy(source, target, in_sem.at[i]) for i, (source, target) in enumerate((
            (v_hbm, v_ref), (h_hbm, h_ref), (rates_hbm, rates_ref), (k_hbm, k_ref), (q_hbm, q_ref)))]
    for load in loads:
        load.start()

    barrier = pltpu.get_barrier_semaphore()
    for step in range(1, n_ctx):
        pl.semaphore_signal(barrier, inc=1, device_id={"ctx": lax.rem(me + step, n_ctx)}, device_id_type=MESH)
    for step in range(1, n_head):
        pl.semaphore_signal(barrier, inc=1, device_id={"head": lax.rem(head + step, n_head)}, device_id_type=MESH)
    loads[0].wait()
    vall[me, :feat, :] = v_ref[...].T
    pl.semaphore_wait(barrier, n_ctx + n_head - 2)

    def slab(piece, owner, send, recv, peer):
        return pltpu.make_async_remote_copy(
            src_ref=piece, dst_ref=piece, send_sem=send, recv_sem=recv.at[owner],
            device_id={"ctx": peer}, device_id_type=MESH)

    def v_copy(owner, peer):
        return slab(vall.at[owner, :feat], owner, v_ssem.at[peer], v_rsem, peer)

    def k_copy(owner, peer):
        return slab(kall.at[owner], owner, k_ssem.at[peer], k_rsem, peer)

    def v_forward(owner):
        return slab(vall.at[owner, :feat], owner, v_fsem.at[owner], v_rsem, partner)

    def k_forward(owner):
        return slab(kall.at[owner], owner, k_fsem.at[owner], k_rsem, partner)

    def v_relay(owner, peer):
        return slab(vall.at[owner, :feat], owner, v_lsem.at[owner], v_rsem, peer)

    def k_relay(owner, peer):
        return slab(kall.at[owner], owner, k_lsem.at[owner], k_rsem, peer)

    square = n_ctx == 8
    v_relays = ((2, 0, 6), (5, 1, 7), (6, 2, 4), (7, 3, 5)) if square else ()
    k_relays = ((2, 0, 6), (5, 1, 7), (7, 3, 5)) if square else ()

    def to_later(copy, action, whole=True):
        if square:
            if not whole:
                @pl.when(me == 2)
                def _():
                    action(copy(me, 4))

            for group, targets in ((0, (1, 2)), (1, (3,)), (2, (3,))):
                @pl.when(me // 2 == group)
                def _():
                    for target in targets:
                        action(copy(me, 2 * target + odd))
        else:
            def go(i, carry):
                action(copy(me, me + 2 * (later_pairs - i)))
                return carry
            lax.fori_loop(0, later_pairs, go, 0)

        @pl.when(odd == 0)
        def _():
            action(copy(me, me + 1))

    def quarter_cols(base, which):
        return pl.ds(pl.multiple_of(base + which * quarter, 128), quarter)

    def w_piece(owner, which):
        return wbuf.at[pl.ds(pl.multiple_of(owner * feat, 128), feat), quarter_cols(0, which)]

    def w_copy(owner, peer):
        return pltpu.make_async_remote_copy(
            src_ref=w_ref.at[:, quarter_cols(peer * width, mine_q)], dst_ref=w_piece(owner, mine_q),
            send_sem=w_ssem.at[peer], recv_sem=w_rsem.at[owner],
            device_id={"head": peer}, device_id_type=MESH)

    def w_hand(owner, which, way, peer):
        return pltpu.make_async_remote_copy(
            src_ref=w_piece(owner, which), dst_ref=w_piece(owner, which),
            send_sem=wf_ssem.at[way, owner], recv_sem=wf_rsem.at[way, owner],
            device_id={"ctx": peer}, device_id_type=MESH)

    beside = mine_q + 1 - 2 * odd
    over = lax.rem(mine_q + 2, share)
    over_beside = lax.rem(beside + 2, share)

    def a_rows(part):
        return pl.ds(part * strip, strip)

    def a_cols(owner):
        return pl.ds(pl.multiple_of(owner * feat, 128), feat)

    def a_copy(owner, peer, part):
        return pltpu.make_async_remote_copy(
            src_ref=att.at[a_rows(part), :], dst_ref=flat_ref.at[a_rows(part), a_cols(owner)],
            send_sem=a_ssem.at[part, peer], recv_sem=a_rsem.at[part, owner],
            device_id={"head": peer}, device_id_type=MESH)

    def a_relay(owner, peer, part):
        piece = flat_ref.at[a_rows(part), a_cols(owner)]
        return pltpu.make_async_remote_copy(
            src_ref=piece, dst_ref=piece,
            send_sem=a_fsem.at[part, owner], recv_sem=a_rsem.at[part, owner],
            device_id={"head": peer}, device_id_type=MESH)

    for step in range(1, n_head):
        w_copy(head, lax.rem(head + step, n_head)).start()
    w_own = pltpu.make_async_copy(
        w_ref.at[:, pl.ds(pl.multiple_of(head * width, 128), width)],
        wbuf.at[pl.ds(pl.multiple_of(head * feat, 128), feat), :], own_sem.at[0])
    w_own.start()

    ri = lax.broadcasted_iota(jnp.int32, (block, block), 0)
    ci = lax.broadcasted_iota(jnp.int32, (block, block), 1)
    eye = ri == ci
    unit = jnp.where(eye, 1.0, 0.0).astype(F32)
    strict = ri < ci
    every = range(blocks)
    parts = [slice(b * block, (b + 1) * block) for b in every]

    def within(fine, coarse):
        return jnp.logical_and((ri >> coarse) == (ci >> coarse), (ri >> fine) != (ci >> fine))

    for load in loads[1:4]:
        load.wait()
    ups, khs, steps = [], [], []
    for b in every:
        hb, kb = h_ref[parts[b], :], k_ref[parts[b], :]
        both = lax.dot_general(jnp.concatenate([hb, kb], 0), hb, NT, preferred_element_type=F32)
        gram = both[:block]
        norm = jnp.sum(jnp.where(eye, gram, 0.0), axis=0, keepdims=True) + EPSILON
        step_row = rates_ref[:, parts[b]] / norm
        steps.append(jnp.sum(jnp.where(eye, step_row, 0.0), axis=1, keepdims=True))
        ups.append(jnp.where(strict, gram * step_row, 0.0))
        khs.append(jnp.where(strict, both[block:], 0.0))

    to_later(v_copy, lambda copy: copy.start(), True)
    loads[4].wait()
    vall[:, feat:, :] = jnp.ones((n_ctx, vall.shape[1] - feat, rows), BF16)

    base = [jnp.where(within(0, 3), u, 0.0) for u in ups]
    bs = [split(u) for u in base]
    squares = [mm3(p, p) for p in bs]
    qs = [split(x) for x in squares]
    cubes = [mm3(bs[b], qs[b]) for b in every]
    fourths = [mm3(qs[b], qs[b]) for b in every]
    firsts = [unit - base[b] + squares[b] - cubes[b] for b in every]
    invs = [firsts[b] + mm3(split(firsts[b]), split(fourths[b])) for b in every]
    size = 3
    while (1 << size) < block:
        top = min(size + 2, block.bit_length() - 1)
        xs = [split(x) for x in invs]
        offs = [split(jnp.where(within(size, top), u, 0.0)) for u in ups]
        zs = [split(mm3(xs[b], offs[b])) for b in every]
        ones = [invs[b] - mm3(zs[b], xs[b]) for b in every]
        if top == size + 2:
            twos = [split(mm3(zs[b], zs[b])) for b in every]
            ones = [ones[b] + mm3(twos[b], split(ones[b])) for b in every]
        invs = ones
        size = top

    for device, owner, peer in v_relays:
        @pl.when(me == device)
        def _():
            v_copy(owner, me).wait_recv()
            v_relay(owner, peer).start()

    rights, groups = [], []
    for b in every:
        hb, kb = h_ref[parts[b], :], k_ref[parts[b], :]
        th, tl = split(invs[b] * steps[b])
        kh, kl = split(khs[b])
        left = jnp.concatenate([kh, hb.T], 0)
        right = mm(twice(left, 1), jnp.concatenate([th, tl], 0))
        right = jnp.concatenate([right[:block] + mm(kl, th), right[block:]], 0)
        rh, rl = split(right)
        rights.append((rh, jnp.concatenate([rh, rl], 1)))
        change = mm(rights[b][1], twice(hb, 0))
        groups.append((kb.astype(F32) - change[:block], unit - change[block:]))

    levels = []
    while len(groups) > 1:
        merged, level = [], []
        for g in range(0, len(groups) - 1, 2):
            (early, early_all), (late, late_all) = groups[g], groups[g + 1]
            joined = jnp.concatenate([early, early_all], 0)
            parted = split(joined)
            level.append(parted[0])
            out = mm3(parted, split(late_all))
            merged.append((jnp.concatenate([out[:-feat], late], 0), out[-feat:]))
        levels.append(level)
        groups = merged
    kall[me, :rows, :] = groups[0][0].astype(BF16)
    kall[me, rows:, :] = groups[0][1].astype(BF16)
    to_later(k_copy, lambda copy: copy.start(), False)

    moving = []
    for b in every:
        hb, kb, qb = h_ref[parts[b], :], k_ref[parts[b], :], q_ref[parts[b], :]
        both = lax.dot_general(jnp.concatenate([hb, kb], 0), qb, NT, preferred_element_type=F32)
        wh, wl = split(jnp.where(ri <= ci, both[:block], 0.0))
        change = mm(rights[b][1], twice(wh, 0)) + mm(rights[b][0], wl)
        inside = (both[block:] - change[:block]) * scale
        near[parts[b], parts[b]] = jnp.where(ri <= ci, inside, NEGATIVE)
        moving.append((qb.T.astype(F32) - change[block:]) * scale)
    width_now = block
    for level in levels:
        joined = []
        for g, keys in enumerate(level):
            first = 2 * g * width_now
            out = mm(twice(keys, 1), jnp.concatenate(split(moving[2 * g + 1]), 0))
            near[first : first + width_now, first + width_now : first + 2 * width_now] = out[:-feat]
            near[first + width_now : first + 2 * width_now, first : first + width_now] = jnp.full(
                (width_now, width_now), NEGATIVE, F32)
            joined.append(jnp.concatenate([moving[2 * g], out[-feat:]], 1))
        moving = joined
        width_now *= 2
    mov[...] = moving[0]
    for t in range(rows // tile):
        cols = slice(t * tile, (t + 1) * tile)
        seen = (t + 1) * tile
        scores = near[:seen, cols]
        top = jnp.max(scores, axis=0, keepdims=True)
        peak[:, cols] = top
        acc[:, cols] = mm(vall[me, :, :seen], jnp.exp2(scores - top).astype(BF16))

    def attend(tiles, sources):
        every_score = []
        for cols in tiles:
            current = mov[:, cols]
            scores = []
            for source in sources:
                out = mm(twice(kall[source], 1), jnp.concatenate(split(current), 0))
                scores.append(out[:rows])
                current = out[rows:]
            mov[:, cols] = current
            every_score.append(scores)
        for cols, scores in zip(tiles, every_score):
            old = peak[:, cols]
            top = old
            for s in scores:
                top = jnp.maximum(top, jnp.max(s, axis=0, keepdims=True))
            peak[:, cols] = top
            gathered = acc[:, cols] * jnp.exp2(old - top)
            for source, s in zip(sources, scores):
                gathered = gathered + mm(vall[source], jnp.exp2(s - top).astype(BF16))
            acc[:, cols] = gathered

    def pass_values(i, carry):
        source = me - 2 - 2 * i
        taken = source < 0
        for device, owner, _ in v_relays:
            taken = jnp.logical_or(taken, jnp.logical_and(me == device, source == owner))

        @pl.when(jnp.logical_not(taken))
        def _():
            v_copy(source, me).wait_recv()
        v_forward(source).start()
        return carry
    lax.fori_loop(0, earlier_pairs, pass_values, 0)

    def relayed(owner, peer):
        if n_head < 3:
            return owner != owner
        return jnp.logical_or(jnp.logical_and(owner == 0, peer == n_head - 1),
                              jnp.logical_and(owner == n_head - 1, peer == 0))

    def direct(part, action):
        for beyond, peers in ((True, range(n_head - 1, 0, -1)), (False, range(n_head - 1))):
            for peer in peers:
                wanted = head < peer if beyond else head > peer

                @pl.when(jnp.logical_and(wanted, jnp.logical_not(relayed(head, peer))))
                def _():
                    action(a_copy(head, peer, part))

    groups_of = [[pl.ds(part * span + t * tile, tile) for t in range(span // tile)] for part in range(halves)]
    for device, owner, peer in k_relays:
        @pl.when(me == device)
        def _():
            k_copy(owner, me).wait_recv()
            k_relay(owner, peer).start()
            k_forward(owner).start()

    for part in range(halves):
        @pl.when(odd == 1)
        def _():
            if part == 0:
                k_copy(me - 1, me).wait_recv()
                v_copy(me - 1, me).wait_recv()
            attend(groups_of[part], [me - 1])

        def visit(i, carry):
            low = (earlier_pairs - 1 - i) * 2
            if part == 0:
                mine, other = low + odd, low + 1 - odd
                taken = mine < 0
                for device, owner, _ in k_relays:
                    taken = jnp.logical_or(taken, jnp.logical_and(me == device, mine == owner))

                @pl.when(jnp.logical_not(taken))
                def _():
                    k_copy(mine, me).wait_recv()
                    k_forward(mine).start()
                k_copy(other, me).wait_recv()
                v_copy(other, me).wait_recv()
            attend(groups_of[part], [low + 1, low])
            return carry

        lax.fori_loop(0, earlier_pairs, visit, 0)
        for cols in groups_of[part]:
            att[cols, :] = (acc[:feat, cols] / acc[feat : feat + 1, cols]).T.astype(BF16)
        for piece in (2 * part, 2 * part + 1):
            direct(piece, lambda copy: copy.start())
        held = pl.ds(part * span, span)
        attended_ref[held, :] = att[held, :]
        flat_ref[held, a_cols(head)] = att[held, :]
        if part == 0:
            for step in range(1, n_head):
                other = lax.rem(head + step, n_head)
                w_copy(other, head).wait_recv()
                w_hand(other, mine_q, 0, partner).start()
                if share == 4:
                    w_hand(other, mine_q, 1, across).start()
            w_own.wait()

    others = [lax.rem(head + step, n_head) for step in range(1, n_head)]
    if share == 4:
        for other in others:
            w_hand(other, over, 1, across).wait_recv()
            w_hand(other, over, 2, partner).start()
        for other in others:
            w_hand(other, over_beside, 2, partner).wait_recv()
    for other in others:
        w_hand(other, beside, 0, partner).wait_recv()

    to_later(v_copy, lambda copy: copy.wait_send(), True)
    to_later(k_copy, lambda copy: copy.wait_send(), False)

    def passed(i, carry):
        source = me - 2 - 2 * i
        v_forward(source).wait_send()
        k_forward(source).wait_send()
        return carry
    lax.fori_loop(0, earlier_pairs, passed, 0)
    for relays, relay_copy in ((v_relays, v_relay), (k_relays, k_relay)):
        for device, owner, peer in relays:
            @pl.when(me == device)
            def _():
                relay_copy(owner, peer).wait_send()

    for step in range(1, n_head):
        other = lax.rem(head + step, n_head)
        w_copy(head, other).wait_send()
        w_hand(other, mine_q, 0, partner).wait_send()
        if share == 4:
            w_hand(other, mine_q, 1, across).wait_send()
            w_hand(other, over, 2, partner).wait_send()

    for part in range(pieces):
        if n_head >= 3:
            for owner, relay, peer in ((0, n_head - 2, n_head - 1), (n_head - 1, 1, 0)):
                @pl.when(head == relay)
                def _():
                    a_copy(owner, relay, part).wait_recv()
                    a_relay(owner, peer, part).start()
        for owner in range(n_head):
            skip = head != owner
            if n_head >= 3 and owner in (0, n_head - 1):
                skip = jnp.logical_and(skip, head != (n_head - 2 if owner == 0 else 1))

            @pl.when(skip)
            def _():
                a_copy(owner, head, part).wait_recv()

        def project(i, carry):
            out_rows = pl.ds(pl.multiple_of(part * strip + (i // strips) * tall, tall), tall)
            out_cols = pl.ds(pl.multiple_of(lax.rem(i, strips) * wide, 128), wide)
            proj_ref[out_rows, out_cols] = mm(flat_ref[out_rows, :], wbuf[:, out_cols]).astype(BF16)
            return carry

        tall, wide = min(256, strip), min(512, width)
        strips = width // wide
        lax.fori_loop(0, (strip // tall) * strips, project, 0)

    for part in range(pieces):
        direct(part, lambda copy: copy.wait_send())
        if n_head >= 3:
            for owner, relay, peer in ((0, n_head - 2, n_head - 1), (n_head - 1, 1, 0)):
                @pl.when(head == relay)
                def _():
                    a_relay(owner, peer, part).wait_send()


def solution(mesh):
    n_ctx, n_head = mesh.shape["ctx"], mesh.shape["head"]

    def body(queries, keys, values, house, rates, out_weight):
        rows, _, feat = queries.shape
        block = feat
        tile = min(256, rows)
        halves = 2 if rows % (2 * tile) == 0 else 1
        width = out_weight.shape[1] // n_head
        vmem = pl.BlockSpec(memory_space=pltpu.VMEM)
        hbm = pl.BlockSpec(memory_space=pltpu.HBM)
        dma = pltpu.SemaphoreType.DMA
        attended, projected = pl.pallas_call(
            functools.partial(kernel, n_ctx, n_head, block, tile, halves),
            out_shape=(
                pltpu.VMEM((rows, feat), BF16),
                pltpu.VMEM((rows, width), BF16),
            ),
            in_specs=[hbm] * 6,
            out_specs=(vmem, vmem),
            scratch_shapes=[pltpu.VMEM((rows, feat), BF16)] * 4 + [
                pltpu.VMEM((1, rows), F32),
                pltpu.VMEM((n_ctx, rows + feat, feat), BF16),
                pltpu.VMEM((n_ctx, feat + 16, rows), BF16),
                pltpu.VMEM((n_head * feat, width), BF16),
                pltpu.VMEM((rows, n_head * feat), BF16),
                pltpu.VMEM((rows, feat), BF16),
                pltpu.VMEM((rows, rows), F32),
                pltpu.VMEM((feat, rows), F32),
                pltpu.VMEM((feat + 16, rows), F32),
                pltpu.VMEM((1, rows), F32),
                dma((n_ctx,)), dma((n_ctx,)), dma((n_ctx,)), dma((n_ctx,)), dma((n_ctx,)), dma((n_ctx,)), dma((n_ctx,)), dma((n_ctx,)),
                dma((n_head,)), dma((n_head,)), dma((3, n_head)), dma((3, n_head)),
                dma((2 * halves, n_head)), dma((2 * halves, n_head)), dma((2 * halves, n_head)), dma((1,)), dma((5,)),
            ],
            compiler_params=pltpu.CompilerParams(
                collective_id=0, has_side_effects=True, vmem_limit_bytes=66 * 1000 * 1000 - 2 * rows * (width + feat)),
            name="path_attention",
        )(queries.reshape(rows, feat), keys.reshape(rows, feat), values.reshape(rows, feat),
          house.reshape(rows, feat), rates, out_weight)
        return attended.reshape(rows, 1, feat), projected

    in_specs = (
        P("ctx", "head", None),
        P("ctx", "head", None),
        P("ctx", "head", None),
        P("ctx", "head", None),
        P("head", "ctx"),
        P("head", None),
    )
    out_specs = (P("ctx", "head", None), P("ctx", "head"))
    return jax.shard_map(body, mesh=mesh, in_specs=in_specs, out_specs=out_specs, check_vma=False)
```
